32 devices in a mesh: group: 4 (over x, core), member: 8 (over z, y).
Axes of the slice: x: 2, y: 2, z: 4, core: 2. Of those that a mesh axis runs over, the one named last changes fastest.
Arguments:
- embedded: bfloat16 [4096, 2048], P(('group', 'member')), may hold values from -6 to 6
- seq_lengths: int32 [32, 4], P(('group', 'member')), may hold values from 1 to 31, as said below
- client_gain: float32 [2048], replicated, may hold values from 0.1 to 1.9
- adapter_down: bfloat16 [2048, 128], P('member'), may hold values from -0.125 to 0.125
- adapter_up: bfloat16 [128, 2048], P(None, 'member'), may hold values from -0.5 to 0.5
- server_gain: float32 [2048], replicated, may hold values from 0.1 to 1.9
- gate_weight: bfloat16 [2048, 4096], P(None, 'group'), may hold values from -0.125 to 0.125
- up_weight: bfloat16 [2048, 4096], P(None, 'group'), may hold values from -0.125 to 0.125
- hidden_grad: bfloat16 [8, 4, 64, 4096], P('member', None, None, 'group'), may hold values from -6 to 6
Outputs:
- input_grad: bfloat16 [4096, 2048], P(('group', 'member'))
- delta_down: float32 [2048, 128], P('member')
- delta_up: float32 [128, 2048], P(None, 'member')
The draws below stay inside these ranges and needn't reach their ends.
Inputs may be any that keep to these rules, and one draw needn't show every extreme that they name: `seq_lengths`: the lengths of one client's sequences sum to at most 64, and some client's lengths sum to exactly 64.
All inputs are finite; a program needn't handle non-finite values.
Results may differ from the reference program's by a relative error of at most 0.025.
Values may be sent and summed in bfloat16 or wider, within the bound.
No kernel may reach another device: no remote copies, remote signals or barrier semaphores. Data moves between devices by JAX's collectives and lax.ppermute only.
A program may use at most 64 MiB of HBM per device.

```python
import math
import jax
import jax.numpy as jnp
from jax import lax

D = 2048
FW = 4096
R = 128
SEQS = 4
BUCKET = 32
SLOTS = 128
CAP = 64
CLIENTS = 32
N_GROUP = 4
N_MEMBER = 8


def draw_seq_lengths(key, part):
    key_first = jax.random.fold_in(key, 11)
    key_second = jax.random.fold_in(key, 12)
    key_pick = jax.random.fold_in(key, 13)
    first = jax.random.randint(key_first, (CLIENTS, SEQS // 2), 1, BUCKET)
    room = BUCKET - first
    second = jax.random.randint(key_second, (CLIENTS, SEQS // 2), 1, room + 1)
    chosen = jax.random.randint(key_pick, (), 0, CLIENTS)
    is_chosen = lax.iota(jnp.int32, CLIENTS)[:, None] == chosen
    second = jnp.where(is_chosen, room, second)
    return jnp.stack([first, second], axis=-1).reshape(CLIENTS, SEQS).astype(jnp.int32)


def levels(rng, shape, split, least, top_value):
    def one(axis_at, parts):
        draws = jax.random.uniform(jax.random.fold_in(jax.random.fold_in(rng, 6), axis_at), (parts,), jnp.float32, least / len(split), top_value / len(split))
        return jnp.repeat(jnp.exp(draws), shape[axis_at] // parts).reshape((-1,) + (1,) * (len(shape) - axis_at - 1))

    level = one(*split[0])
    for cut in split[1:]:
        level = level * one(*cut)
    return level


def normal_values(stream_key, dims, spread, most, split=(), kind=jnp.bfloat16):
    values = jax.random.normal(stream_key, dims, jnp.float32) * spread
    if len(split) > 0:
        values = levels(stream_key, dims, split, -0.22, 0.18) * values
    return jnp.clip(values, min=-most, max=most).astype(kind)


def setup_inputs(seed: int = 0) -> dict:
    splits = jax.random.split(jax.random.key(seed), 10)
    embedded = normal_values(splits[0], (CLIENTS * SLOTS, D), 1.0, 6.0, ((0, 32),))
    seq_lengths = draw_seq_lengths(jax.random.fold_in(splits[9], 71), 0)
    client_gain = jnp.clip(1.0 + 0.18 * jax.random.normal(splits[2], (D,), jnp.float32), 0.1, 1.9)
    adapter_down = normal_values(splits[3], (D, R), D ** -0.5, 0.125, ((0, 8),))
    adapter_up = normal_values(splits[4], (R, D), R ** -0.5, 0.5, ((1, 8),))
    server_gain = jnp.clip(1.0 + 0.18 * jax.random.normal(splits[5], (D,), jnp.float32), 0.1, 1.9)
    gate_weight = normal_values(splits[6], (D, FW), D ** -0.5, 0.125, ((1, 4),))
    up_weight = normal_values(splits[7], (D, FW), D ** -0.5, 0.125, ((1, 4),))
    hidden_grad = normal_values(splits[8], (N_MEMBER, N_GROUP, CAP, FW), 1.0, 6.0, ((0, 8), (3, 4)))
    return {"embedded": embedded, "seq_lengths": seq_lengths, "client_gain": client_gain, "adapter_down": adapter_down, "adapter_up": adapter_up, "server_gain": server_gain, "gate_weight": gate_weight, "up_weight": up_weight, "hidden_grad": hidden_grad}


def normalize(values, gain_vec):
    values = values.astype(jnp.float32)
    inverse = lax.rsqrt(lax.optimization_barrier(jnp.mean(values * values, axis=-1, keepdims=True)) + 1e-05)
    return values * inverse * gain_vec

def selector(lengths_row, slot_count, capacity, bucket, seq_count):
    slot_ids = lax.iota(jnp.int32, slot_count)
    seq_of = slot_ids // bucket
    within = slot_ids % bucket
    matches = seq_of[:, None] == lax.iota(jnp.int32, seq_count)[None, :]
    before = jnp.cumsum(lengths_row) - lengths_row
    own_len = lax.optimization_barrier(jnp.sum(jnp.where(matches, lengths_row[None, :], 0), axis=1))
    own_start = lax.optimization_barrier(jnp.sum(jnp.where(matches, before[None, :], 0), axis=1))
    dest_row = (own_start + within).astype(jnp.int32)
    is_live = within < own_len
    chooser = (lax.iota(jnp.int32, capacity)[:, None] == dest_row[None, :]) & is_live[None, :]
    return chooser.astype(jnp.bfloat16)

def gated_grads(gate_value, up_value, upstream):
    sigmoid = jax.nn.sigmoid(gate_value)
    grad_gate = upstream * up_value * sigmoid * (1.0 + gate_value * (1.0 - sigmoid))
    grad_up = upstream * gate_value * sigmoid
    return (grad_gate.astype(jnp.bfloat16), grad_up.astype(jnp.bfloat16))

def reference(embedded, seq_lengths, client_gain, adapter_down, adapter_up, server_gain, gate_weight, up_weight, hidden_grad):
    blocks = embedded.reshape(N_GROUP, N_MEMBER, SLOTS, D).transpose(1, 0, 2, 3)
    lens = seq_lengths.reshape(N_GROUP, N_MEMBER, SEQS).transpose(1, 0, 2)
    share = FW // N_GROUP

    def client_forward(rows, lengths_row):
        normed = normalize(rows, client_gain).astype(jnp.bfloat16)
        low_rank = jnp.dot(normed, adapter_down, preferred_element_type=jnp.float32).astype(jnp.bfloat16)
        cut_rows = (rows.astype(jnp.float32) + jnp.dot(low_rank, adapter_up, preferred_element_type=jnp.float32)).astype(jnp.bfloat16)
        chooser = selector(lengths_row, SLOTS, CAP, BUCKET, SEQS)
        packed = jnp.dot(chooser, cut_rows, preferred_element_type=jnp.float32).astype(jnp.bfloat16)
        return (normed, low_rank, chooser, packed)

    def client_backward(rows, normed, low_rank, chooser, packed, d_server):
        pullback = jax.vjp(lambda v: normalize(v, server_gain), packed.astype(jnp.float32))[1]
        d_packed = pullback(d_server)[0].astype(jnp.bfloat16)
        d_cut = lax.dot_general(chooser, d_packed, (((0,), (0,)), ((), ())), preferred_element_type=jnp.float32).astype(jnp.bfloat16)
        up_term = lax.dot_general(low_rank, d_cut, (((0,), (0,)), ((), ())), preferred_element_type=jnp.float32)
        d_low = lax.dot_general(d_cut, adapter_up, (((1,), (1,)), ((), ())), preferred_element_type=jnp.float32).astype(jnp.bfloat16)
        down_term = lax.dot_general(normed, d_low, (((0,), (0,)), ((), ())), preferred_element_type=jnp.float32)
        d_normed = lax.dot_general(d_low, adapter_down, (((1,), (1,)), ((), ())), preferred_element_type=jnp.float32)
        pull_client = jax.vjp(lambda v: normalize(v, client_gain), rows.astype(jnp.float32))[1]
        grads = (d_cut.astype(jnp.float32) + pull_client(d_normed)[0]).astype(jnp.bfloat16)
        return (grads, down_term, up_term)

    def column(operands):
        rows_all, lens_all, upstream = operands
        normed, low_rank, chooser, packed = jax.vmap(client_forward)(rows_all, lens_all)
        server_in = normalize(packed, server_gain).astype(jnp.bfloat16).reshape(N_GROUP * CAP, D)
        gate_value = jnp.dot(server_in, gate_weight, preferred_element_type=jnp.float32)
        up_value = jnp.dot(server_in, up_weight, preferred_element_type=jnp.float32)
        grad_gate, grad_up = gated_grads(gate_value, up_value, upstream.reshape(N_GROUP * CAP, FW).astype(jnp.float32))
        d_server = jnp.zeros((N_GROUP * CAP, D), jnp.float32)
        for block in range(N_GROUP):
            lower = block * share
            upper = lower + share
            partial_sum = lax.dot_general(grad_gate[:, lower:upper], gate_weight[:, lower:upper], (((1,), (1,)), ((), ())), preferred_element_type=jnp.float32)
            partial_sum = partial_sum + lax.dot_general(grad_up[:, lower:upper], up_weight[:, lower:upper], (((1,), (1,)), ((), ())), preferred_element_type=jnp.float32)
            d_server = d_server + partial_sum.astype(jnp.bfloat16).astype(jnp.float32)
        d_server = d_server.reshape(N_GROUP, CAP, D)
        grads, downs, ups = jax.vmap(client_backward)(rows_all, normed, low_rank, chooser, packed, d_server)
        return (grads, lax.optimization_barrier(jnp.sum(downs, axis=0)), lax.optimization_barrier(jnp.sum(ups, axis=0)))
    grads, downs, ups = lax.map(column, (blocks, lens, hidden_grad))
    input_grad = grads.transpose(1, 0, 2, 3).reshape(N_GROUP * N_MEMBER * SLOTS, D)
    divisor = 8.0 * math.sqrt(float(N_GROUP * N_MEMBER))
    return (input_grad, lax.optimization_barrier(jnp.sum(downs, axis=0)) / divisor, lax.optimization_barrier(jnp.sum(ups, axis=0)) / divisor)
```

```python
import math

import jax
import jax.numpy as jnp
from jax import lax
from jax.sharding import PartitionSpec as P

F32, BF16 = jnp.float32, jnp.bfloat16


def selector(lengths_row, slot_count, capacity, bucket, seq_count):
    slot_ids = lax.iota(jnp.int32, slot_count)
    within = slot_ids % bucket
    own_len = jnp.zeros((slot_count,), jnp.int32)
    own_start = jnp.zeros((slot_count,), jnp.int32)
    start = jnp.int32(0)
    for s in range(seq_count):
        here = slot_ids // bucket == s
        own_len = jnp.where(here, lengths_row[s], own_len)
        own_start = jnp.where(here, start, own_start)
        start = start + lengths_row[s]
    dest_row = own_start + within
    is_live = within < own_len
    chooser = (lax.iota(jnp.int32, capacity)[:, None] == dest_row[None, :]) & is_live[None, :]
    return chooser.astype(BF16)


def inverse_rms(values):
    return lax.rsqrt(jnp.mean(values * values, axis=-1, keepdims=True) + 1e-05)


def norm_grad(values, inverse, gain, upstream):
    scaled = upstream * gain
    along = jnp.mean(scaled * values, axis=-1, keepdims=True)
    return inverse * (scaled - values * (inverse * inverse * along))


def dot(a, b, dims, out=F32):
    return lax.dot_general(a, b, (dims, ((), ())), preferred_element_type=F32).astype(out)


NN, NT, TN = ((1,), (0,)), ((1,), (1,)), ((0,), (0,))


def body(embedded, seq_lengths, client_gain, adapter_down, adapter_up, server_gain, gate_weight, up_weight, hidden_grad):
    slot_count, width = embedded.shape
    seq_count = seq_lengths.shape[1]
    capacity = hidden_grad.shape[2]
    share, rank = adapter_down.shape
    hidden = gate_weight.shape[1]
    groups = lax.axis_size("group")
    members = lax.axis_size("member")
    n_rest, n_z = groups // 2, members // 2
    group, member = lax.axis_index("group"), lax.axis_index("member")
    rest, core = group // 2, group % 2
    z, y = member // 2, member % 2

    def swap_core(v):
        return lax.ppermute(v, "group", [(i, i ^ 1) for i in range(groups)])

    def swap_y(v):
        return lax.ppermute(v, "member", [(i, i ^ 1) for i in range(members)])

    def shift_rest(v, k):
        return lax.ppermute(v, "group", [(i, (i + 2 * k) % groups) for i in range(groups)])

    def shift_z(v, k):
        return lax.ppermute(v, "member", [(i, (i + 2 * k) % members) for i in range(members)])

    half = share // 2
    down_half = lax.dynamic_slice_in_dim(adapter_down, core * half, half, 0)
    up_half = lax.dynamic_slice_in_dim(adapter_up.T, core * half, half, 0)
    piece = jnp.stack([down_half, up_half])
    own_y = jnp.stack([piece] + [shift_z(piece, k) for k in range(1, n_z)])
    other_y = swap_y(own_y)
    own_core = jnp.stack([own_y, other_y])
    other_core = swap_core(own_core)
    both = jnp.stack([own_core, other_core])
    both = jnp.where(core == 0, both, both[::-1])
    both = jnp.where(y == 0, both, both[:, ::-1])
    both = jnp.flip(both, 2)
    both = lax.dynamic_slice_in_dim(jnp.concatenate([both, both], 2), n_z - 1 - z, n_z, 2)
    both = both.transpose(3, 2, 1, 0, 4, 5).reshape(2, width, rank)
    full_down, full_up = both[0], both[1]

    chooser = selector(seq_lengths[0], slot_count, capacity, slot_count // seq_count, seq_count)
    mine = dot(chooser, embedded, NN, BF16)
    same = [mine] + [shift_rest(mine, k) for k in range(1, n_rest)]
    rows = jnp.concatenate(same + [swap_core(v) for v in same], 0)

    rows32 = rows.astype(F32)
    client_inv = inverse_rms(rows32)
    normed = (rows32 * client_inv * client_gain).astype(BF16)
    low_rank = dot(normed, full_down, NN, BF16)
    packed = (rows32 + dot(low_rank, full_up, NT)).astype(BF16)
    packed32 = packed.astype(F32)
    server_inv = inverse_rms(packed32)
    server_in = (packed32 * server_inv * server_gain).astype(BF16)

    gate = dot(server_in, gate_weight, NN)
    up = dot(server_in, up_weight, NN)
    order = [((rest - k) % n_rest) * 2 + (core ^ d) for d in range(2) for k in range(n_rest)]
    upstream = jnp.concatenate(
        [lax.dynamic_slice_in_dim(hidden_grad[0], o, 1, 0).reshape(capacity, hidden) for o in order], 0
    ).astype(F32)
    sig = jax.nn.sigmoid(gate)
    grad_gate = (upstream * up * sig * (1.0 + gate * (1.0 - sig))).astype(BF16)
    grad_up = (upstream * gate * sig).astype(BF16)
    partial = dot(grad_gate, gate_weight, NT) + dot(grad_up, up_weight, NT)

    sent = swap_core(partial[n_rest * capacity :].astype(BF16))
    pair = partial[: n_rest * capacity] + sent.astype(F32)
    d_server = pair[:capacity]
    for k in range(1, n_rest):
        d_server = d_server + shift_rest(pair[k * capacity : (k + 1) * capacity].astype(BF16), n_rest - k).astype(F32)
    mine32, mine_inv = rows32[:capacity], client_inv[:capacity]
    d_packed = norm_grad(packed32[:capacity], server_inv[:capacity], server_gain, d_server).astype(BF16)
    d_low = dot(d_packed, full_up, NN, BF16)
    d_normed = dot(d_low, full_down, NT)
    grads = (d_packed.astype(F32) + norm_grad(mine32, mine_inv, client_gain, d_normed)).astype(BF16)
    input_grad = dot(chooser, grads, TN, BF16)

    d_part = norm_grad(packed32, server_inv, server_gain, partial).astype(BF16)
    low_part = dot(d_part, full_up, NN, BF16)
    down_term = dot(normed, low_part, TN)
    up_term = dot(d_part, low_rank, TN)
    keep = jnp.where(core == 0, down_term, up_term)
    give = jnp.where(core == 0, up_term, down_term)
    total = keep + swap_core(give.astype(BF16)).astype(F32)
    total = total.reshape(n_z, 2, share, rank)
    keep = jnp.where(y == 0, total[:, 0], total[:, 1])
    give = jnp.where(y == 0, total[:, 1], total[:, 0])
    total = keep + swap_y(give.astype(BF16)).astype(F32)
    block = lax.dynamic_index_in_dim(total, z, 0, keepdims=False)
    for k in range(1, n_z):
        other = lax.dynamic_index_in_dim(total, (z + k) % n_z, 0, keepdims=False)
        block = block + shift_z(other.astype(BF16), k).astype(F32)
    summed = block
    for k in range(1, n_rest):
        summed = summed + shift_rest(block.astype(BF16), k).astype(F32)
    summed = summed / (8.0 * math.sqrt(float(groups * members)))
    swapped = swap_core(summed)
    delta_down = jnp.where(core == 0, summed, swapped)
    delta_up = jnp.where(core == 0, swapped, summed).T
    return (input_grad, delta_down, delta_up)


def solution(mesh):
    in_specs = (
        P(("group", "member"), None),
        P(("group", "member"), None),
        P(),
        P("member", None),
        P(None, "member"),
        P(),
        P(None, "group"),
        P(None, "group"),
        P("member", None, None, "group"),
    )
    out_specs = (P(("group", "member"), None), P("member", None), P(None, "member"))
    return jax.shard_map(body, mesh=mesh, in_specs=in_specs, out_specs=out_specs, check_vma=False)
```

```python
import functools
import math

import jax
import jax.numpy as jnp
from jax import lax
from jax.experimental import pallas as pl
from jax.experimental.pallas import tpu as pltpu
from jax.sharding import PartitionSpec as P


F32, BF16 = jnp.float32, jnp.bfloat16
VMEM = pl.BlockSpec(memory_space=pltpu.VMEM)
HBM = pl.BlockSpec(memory_space=pltpu.HBM)
SMEM = pl.BlockSpec(memory_space=pltpu.SMEM)
TILE, MAIN_BASE = 256, 16 << 20
NN, NT, TN = ((1,), (0,)), ((1,), (1,)), ((0,), (0,))


def dot(a, b, dims, out=F32):
    return lax.dot_general(a, b, (dims, ((), ())), preferred_element_type=F32).astype(out)


def inverse_rms(values):
    return lax.rsqrt(jnp.mean(values * values, axis=-1, keepdims=True) + 1e-05)


def norm_grad(values, inverse, gain, upstream):
    scaled = upstream * gain
    along = jnp.mean(scaled * values, axis=-1, keepdims=True)
    return inverse * (scaled - values * (inverse * inverse * along))


def selector(lengths, capacity, slots, seq_count):
    bucket = slots // seq_count
    slot = lax.broadcasted_iota(jnp.int32, (capacity, slots), 1)
    row = lax.broadcasted_iota(jnp.int32, (capacity, slots), 0)
    chosen = slot < 0
    start = jnp.int32(0)
    for s in range(seq_count):
        length = lengths[0, s]
        within = slot - s * bucket
        chosen |= (within >= 0) & (within < length) & (row == start + within)
        start = start + length
    return jnp.where(chosen, 1.0, 0.0).astype(BF16)


def prepare_kernel(
    where_ref, lengths_ref, embedded_ref, down_ref, up_ref, gains_in, gains2_in, mine_ref, piece_ref, whole_ref, gain_ref, gain2_ref, *, seq_count
):
    core = where_ref[1]
    half = piece_ref.shape[1]
    gain_ref[...] = gains_in[...]
    gain2_ref[...] = gains2_in[...]
    whole_ref[0] = down_ref[...]
    whole_ref[1] = up_ref[...].astype(F32).T.astype(BF16)
    at = pl.ds(pl.multiple_of(core * half, half), half)
    piece_ref[...] = whole_ref[:, at, :]
    chooser = selector(lengths_ref, mine_ref.shape[0], embedded_ref.shape[0], seq_count)
    mine_ref[...] = dot(chooser, embedded_ref[...], NN, BF16)


def main_kernel(where_ref, *refs, groups, n_z, tile):
    n_pieces = 2 * n_z + 3 if n_z > 1 else 3
    rows_refs = refs[:groups]
    piece_refs = refs[groups : groups + n_pieces]
    (client_gain_ref, server_gain_ref, gate_hbm, up_hbm, hidden_hbm,
     down_ref, rise_ref, own_ref, keep_part_ref, give_part_ref, keep_ref, give_ref,
     normed, low, packed, inverse, entering, total, terms, gate_ref, up_ref, hidden_ref, arrived) = refs[groups + n_pieces :]
    fetches = []
    for step in range(gate_ref.shape[1] // tile):
        cols = pl.ds(step * tile, tile)
        fetches.append([
            pltpu.make_async_copy(gate_hbm.at[:, cols], gate_ref.at[:, cols], arrived.at[step, 0]),
            pltpu.make_async_copy(up_hbm.at[:, cols], up_ref.at[:, cols], arrived.at[step, 1]),
            pltpu.make_async_copy(hidden_hbm.at[:, :, cols], hidden_ref.at[:, :, cols], arrived.at[step, 2]),
        ])
        for copy in fetches[-1]:
            copy.start()
    rest, core, z, y = (where_ref[i] for i in range(4))
    n_rest = groups // 2
    capacity = rows_refs[0].shape[0]
    share, _ = piece_refs[0].shape[1:]
    half = share // 2

    def place(ref, dz, dy, part=None):
        holder = lax.rem(z + dz + n_z, n_z) * 2 + (y ^ dy)
        rows, start = (share, holder * share) if part is None else (half, holder * share + part * half)
        at = pl.ds(pl.multiple_of(start, rows), rows)
        down_ref[at, :] = ref[0]
        rise_ref[at, :] = ref[1]

    place(piece_refs[0], 0, 0)
    place(piece_refs[1], 0, 1, core)
    place(piece_refs[2], 0, 1, 1 - core)
    at_piece = 3
    for dy in range(2):
        for k in range(1, n_z // 2):
            place(piece_refs[at_piece], (2 * core - 1) * k, dy)
            place(piece_refs[at_piece + 1], (1 - 2 * core) * k, dy)
            at_piece += 2
        if n_z > 1:
            place(piece_refs[at_piece], n_z // 2, dy, core)
            place(piece_refs[at_piece + 1], n_z // 2, dy, 1 - core)
            at_piece += 2
    for j in range(groups):
        at = pl.ds(j * capacity, capacity)
        rows = rows_refs[j][...].astype(F32)
        normed[at, :] = (rows * inverse_rms(rows) * client_gain_ref[...]).astype(BF16)
    low[...] = dot(normed[...], down_ref[...], NN, BF16)
    for j in range(groups):
        at = pl.ds(j * capacity, capacity)
        cut = (rows_refs[j][...].astype(F32) + dot(low[at, :], rise_ref[...], NT)).astype(BF16)
        packed[at, :] = cut
        cut = cut.astype(F32)
        inv = inverse_rms(cut)
        inverse[at, :] = inv
        entering[at, :] = (cut * inv * server_gain_ref[...]).astype(BF16)
    own_ref[...] = packed[:capacity, :]

    for step in range(gate_ref.shape[1] // tile):
        cols = pl.ds(step * tile, tile)
        for copy in fetches[step]:
            copy.wait()
        gate = dot(entering[...], gate_ref[:, cols], NN)
        up = dot(entering[...], up_ref[:, cols], NN)
        grad_gate, grad_up = [], []
        for j in range(groups):
            d, k = divmod(j, n_rest)
            holder = lax.rem(rest - k + n_rest, n_rest) * 2 + (core ^ d)
            upstream = hidden_ref[holder, :, cols].astype(F32)
            g = gate[j * capacity : (j + 1) * capacity]
            u = up[j * capacity : (j + 1) * capacity]
            sig = jax.nn.sigmoid(g)
            hs = upstream * sig
            grad_gate.append((hs * u * (1.0 + g * (1.0 - sig))).astype(BF16))
            grad_up.append((hs * g).astype(BF16))
        part = dot(jnp.concatenate(grad_gate, 0), gate_ref[:, cols], NT)
        part += dot(jnp.concatenate(grad_up, 0), up_ref[:, cols], NT)
        if step == 0:
            total[...] = part
        else:
            total[...] += part

    for j in range(groups):
        at = pl.ds(j * capacity, capacity)
        upstream = total[at, :]
        d, k = divmod(j, n_rest)
        out = (keep_part_ref, give_part_ref)[d]
        out[pl.ds(k * capacity, capacity), :] = upstream.astype(BF16)
        d_part = norm_grad(packed[at, :].astype(F32), inverse[at, :], server_gain_ref[...], upstream)
        packed[at, :] = d_part.astype(BF16)
    d_part = packed[...]
    low_part = dot(d_part, rise_ref[...], NN, BF16)
    terms[0] = dot(low_part, normed[...], TN).T
    terms[1] = dot(low[...], d_part, TN).T
    for v in range(2):
        for k in range(n_z):
            holder = lax.rem(z + k, n_z) * 2 + (y ^ v)
            at = pl.ds(pl.multiple_of(holder * share, share), share)
            keep_ref[v, k] = terms[core, at, :]
            give_ref[v, k] = terms[1 - core, at, :].astype(BF16)


def client_kernel(lengths_ref, *refs, seq_count, n_rest):
    part_refs = refs[: n_rest + 1]
    (mine_ref, packed_ref, client_gain_ref, server_gain_ref, down_ref, rise_ref, out_ref) = refs[n_rest + 1 :]
    capacity = mine_ref.shape[0]
    d_server = part_refs[0][...].astype(F32)
    for ref in part_refs[1:]:
        d_server = d_server + ref[...].astype(F32)
    packed = packed_ref[...].astype(F32)
    d_packed = norm_grad(packed, inverse_rms(packed), server_gain_ref[...], d_server).astype(BF16)
    d_low = dot(d_packed, rise_ref[...], NN, BF16)
    d_normed = dot(d_low, down_ref[...], NT)
    mine = mine_ref[...].astype(F32)
    grads = d_packed.astype(F32) + norm_grad(mine, inverse_rms(mine), client_gain_ref[...], d_normed)
    chooser = selector(lengths_ref, capacity, out_ref.shape[0], seq_count)
    out_ref[...] = dot(chooser, grads.astype(BF16), TN, BF16)


def finish_kernel(where_ref, own_ref, other_ref, down_ref, up_ref):
    first = where_ref[1] == 0
    own, other = own_ref[...], other_ref[...]
    down_ref[...] = jnp.where(first, own, other)
    up_ref[...] = jnp.where(first, other, own).T


def inner(embedded, seq_lengths, client_gain, adapter_down, adapter_up, server_gain, gate_weight, up_weight, hidden_grad):
    slots, width = embedded.shape
    seq_count = seq_lengths.shape[1]
    capacity = hidden_grad.shape[2]
    share, rank = adapter_down.shape
    hidden = gate_weight.shape[1]
    groups = lax.axis_size("group")
    members = lax.axis_size("member")
    n_rest, n_z = groups // 2, members // 2
    group, member = lax.axis_index("group"), lax.axis_index("member")
    rest, core = group // 2, group % 2
    z, y = member // 2, member % 2
    client_gain, server_gain = client_gain.reshape(1, width), server_gain.reshape(1, width)

    def in_hbm(v):
        return pltpu.with_memory_space_constraint(v, pltpu.HBM)

    def swap_core(v):
        return lax.ppermute(v, "group", [(i, i ^ 1) for i in range(groups)])

    def swap_y(v):
        return lax.ppermute(v, "member", [(i, i ^ 1) for i in range(members)])

    def shift_rest(v, k):
        return lax.ppermute(v, "group", [(i, (i + 2 * k) % groups) for i in range(groups)])

    def shift_z(v, k):
        return lax.ppermute(v, "member", [(i, (i + 2 * k) % members) for i in range(members)])

    half = share // 2
    where = jnp.stack([rest, core, z, y])
    sds = jax.ShapeDtypeStruct
    mine, piece, whole, client_gain, server_gain = pl.pallas_call(
        functools.partial(prepare_kernel, seq_count=seq_count),
        out_shape=(
            sds((capacity, width), BF16),
            sds((2, half, rank), BF16),
            sds((2, share, rank), BF16),
            sds((1, width), F32),
            sds((1, width), F32),
        ),
        in_specs=[SMEM, SMEM] + [VMEM] * 5,
        out_specs=(VMEM,) * 5,
        cost_estimate=pl.CostEstimate(
            flops=2 * capacity * slots * width, bytes_accessed=2 * (slots + capacity) * width, transcendentals=0),
        compiler_params=pltpu.CompilerParams(vmem_limit_bytes=8 << 20),
        name="prepare",
    )(where, *(in_hbm(v) for v in (seq_lengths, embedded, adapter_down, adapter_up, client_gain, server_gain)))

    def shift_pair(v, k):
        pairs = []
        for g in range(groups):
            for m in range(members):
                shift = 2 * k if g % 2 == 0 else members - 2 * k
                pairs.append((g * members + m, g * members + (m + shift) % members))
        return lax.ppermute(v, ("group", "member"), pairs)

    moved = []
    for k in range(1, n_z // 2):
        moved.append(shift_pair(whole, k))
    if n_z > 1:
        moved.append(shift_z(piece, n_z // 2))
    crossed = [swap_y(piece)]
    for v in moved:
        crossed.append(swap_y(v))
    pieces = [whole]
    for v in [crossed[0]] + moved + crossed[1:]:
        pieces += [v, swap_core(v)]

    same = [mine]
    for k in range(1, n_rest):
        same.append(shift_rest(mine, k))
    rows = list(same)
    for k in range(n_rest):
        rows.append(swap_core(same[k]))

    total_rows = groups * capacity
    full_down, full_rise, packed, keep_part, give_part, keep, give = pl.pallas_call(
        functools.partial(main_kernel, groups=groups, n_z=n_z, tile=min(TILE, hidden)),
        out_shape=(
            sds((width, rank), BF16),
            sds((width, rank), BF16),
            sds((capacity, width), BF16),
            sds((n_rest * capacity, width), BF16),
            sds((n_rest * capacity, width), BF16),
            sds((2, n_z, share, rank), F32),
            sds((2, n_z, share, rank), BF16),
        ),
        in_specs=[SMEM] + [VMEM] * (groups + len(pieces) + 2) + [HBM] * 3,
        out_specs=(VMEM,) * 7,
        scratch_shapes=[
            pltpu.VMEM((total_rows, width), BF16),
            pltpu.VMEM((total_rows, rank), BF16),
            pltpu.VMEM((total_rows, width), BF16),
            pltpu.VMEM((total_rows, 1), F32),
            pltpu.VMEM((total_rows, width), BF16),
            pltpu.VMEM((total_rows, width), F32),
            pltpu.VMEM((2, width, rank), F32),
            pltpu.VMEM((width, hidden), BF16),
            pltpu.VMEM((width, hidden), BF16),
            pltpu.VMEM((groups, capacity, hidden), BF16),
            pltpu.SemaphoreType.DMA((hidden // min(TILE, hidden), 3)),
        ],
        compiler_params=pltpu.CompilerParams(
            vmem_limit_bytes=min(60 << 20, MAIN_BASE + 20 * total_rows * width + 4 * width * hidden)),
        cost_estimate=pl.CostEstimate(
            flops=total_rows * width * (8 * hidden + 10 * rank),
            bytes_accessed=4 * width * hidden,
            transcendentals=total_rows * hidden),
        name="main",
    )(
        where, *rows, *pieces, client_gain, server_gain,
        in_hbm(gate_weight), in_hbm(up_weight), in_hbm(hidden_grad.reshape(groups, capacity, hidden)))

    got = swap_core(give)
    other = swap_y((keep[1] + got[1].astype(F32)).astype(BF16))
    sums = keep[0] + got[0].astype(F32) + other.astype(F32)
    block = sums[0]
    for k in range(1, n_z):
        block = block + shift_z(sums[k].astype(BF16), k).astype(F32)
    summed = block
    for k in range(1, n_rest):
        summed = summed + shift_rest(block.astype(BF16), k).astype(F32)
    summed = summed / (8.0 * math.sqrt(float(groups * members)))
    swapped = swap_core(summed)
    delta_down, delta_up = pl.pallas_call(
        finish_kernel,
        out_shape=(sds((share, rank), F32), sds((rank, share), F32)),
        in_specs=[SMEM, VMEM, VMEM],
        out_specs=(VMEM, VMEM),
        compiler_params=pltpu.CompilerParams(vmem_limit_bytes=4 << 20),
        name="finish",
    )(where, summed, swapped)

    sent = swap_core(give_part)
    pair = [
        (keep_part[k * capacity : (k + 1) * capacity].astype(F32)
         + sent[k * capacity : (k + 1) * capacity].astype(F32)).astype(BF16)
        for k in range(1, n_rest)
    ]
    parts = [keep_part[:capacity], sent[:capacity]]
    for k, v in enumerate(pair):
        parts.append(shift_rest(v, n_rest - 1 - k))
    input_grad = pl.pallas_call(
        functools.partial(client_kernel, seq_count=seq_count, n_rest=n_rest),
        out_shape=sds((slots, width), BF16),
        in_specs=[SMEM] + [VMEM] * (n_rest + 7),
        out_specs=VMEM,
        cost_estimate=pl.CostEstimate(
            flops=8 * capacity * rank * width, bytes_accessed=8 * slots * width, transcendentals=0),
        compiler_params=pltpu.CompilerParams(vmem_limit_bytes=16 << 20),
        name="client",
    )(in_hbm(seq_lengths), *parts, mine, packed, client_gain, server_gain, full_down, full_rise)
    return (input_grad, delta_down, delta_up)


def solution(mesh):
    in_specs = (
        P(("group", "member"), None),
        P(("group", "member"), None),
        P(),
        P("member", None),
        P(None, "member"),
        P(),
        P(None, "group"),
        P(None, "group"),
        P("member", None, None, "group"),
    )
    out_specs = (P(("group", "member"), None), P("member", None), P(None, "member"))
    return jax.shard_map(inner, mesh=mesh, in_specs=in_specs, out_specs=out_specs, check_vma=False)
```
